256 devices in a mesh: mem: 16 (over z, core), ma: 16 (over x, y).
Axes of the slice: x: 4, y: 4, z: 8, core: 2. Of those that a mesh axis runs over, the one named last changes fastest.
Arguments:
- ar_state: float32 [3, 64, 128, 2, 1280], P(None, 'mem', 'ma'), may hold values from -4 to 4
- forcing: float32 [3, 64, 128, 2, 1280], P(None, 'mem', 'ma'), may hold values from -6 to 6
- ar_decay: float32 [3], replicated, may hold values from 0.3 to 0.95
- amplitude: float32 [3, 1280], replicated, may hold values from 0.05 to 0.4
- wavenumber: int32 [128], replicated, may hold values from 0 to 1279, as said below
- tables: bfloat16 [128, 1280, 1280], P('ma', None, 'mem'), may hold values from -0.15625 to 0.15625
- tendencies: bfloat16 [64, 1280, 5120], P('mem', 'ma'), may hold values from -6 to 6
Outputs:
- perturbed: bfloat16 [64, 1280, 5120], P('mem', 'ma')
- new_state: float32 [3, 64, 128, 2, 1280], P(None, 'mem', 'ma')
The draws below stay inside these ranges and needn't reach their ends.
Inputs may be any that keep to these rules, and one draw needn't show every extreme that they name: `wavenumber`: 128 distinct values.
All inputs are finite; a program needn't handle non-finite values.
Results may differ from the reference program's by a relative error of at most 0.0042.
Values may be sent and summed in bfloat16 or wider, within the bound.
No kernel may reach another device: no remote copies, remote signals or barrier semaphores. Data moves between devices by JAX's collectives and lax.ppermute only.
A program may use at most 64 MiB of HBM per device.

```python
import math
import jax
import jax.numpy as jnp
from jax import lax

MWIN = 128
NDEG = 1280
NLON = 5120
SCALES = 3
MEMBERS = 64
NLAT = 1280


def draw_wavenumber(key, part):
    return jax.random.permutation(key, NDEG)[:MWIN].astype(jnp.int32)


def steps_of(rng, extent, shards, low, largest):
    loudness, own = 1.0, jax.random.fold_in(rng, 6)
    for axis_at, shards_of in shards:
        draws = jnp.exp(jax.random.uniform(jax.random.fold_in(own, axis_at), (shards_of,), jnp.float32, low / len(shards), largest / len(shards)))
        loudness = loudness * jnp.repeat(draws, extent[axis_at] // shards_of).reshape([-1 if axis == axis_at else 1 for axis in range(len(extent))])
    return loudness


def scatter_about(rng, shape, scale, most, pieces=(), kind=jnp.bfloat16):
    values = scale * jax.random.normal(rng, shape, jnp.float32)
    if pieces:
        values = values * steps_of(rng, shape, pieces, -0.22, 0.18)
    return jnp.clip(values, -most, most).astype(kind)


def setup_inputs(seed: int = 0) -> dict:
    streams_of = jax.random.split(jax.random.key(seed), 8)
    return {
        "ar_state": scatter_about(streams_of[0], (SCALES, MEMBERS, MWIN, 2, NDEG), 0.5, 4.0, ((1, 16), (2, 16)), jnp.float32),
        "forcing": scatter_about(streams_of[1], (SCALES, MEMBERS, MWIN, 2, NDEG), 1.0, 6.0, ((1, 16), (2, 16)), jnp.float32),
        "ar_decay": jnp.clip(jnp.exp(jax.random.uniform(streams_of[2], (SCALES,), jnp.float32, math.log(0.3), math.log(0.95))), 0.3, 0.95),
        "amplitude": jnp.clip(jnp.exp(jax.random.uniform(streams_of[3], (SCALES, NDEG), jnp.float32, math.log(0.05), math.log(0.4))), 0.05, 0.4),
        "wavenumber": draw_wavenumber(jax.random.fold_in(streams_of[7], 71), 0),
        "tables": scatter_about(streams_of[5], (MWIN, NDEG, NLAT), NDEG ** -0.5, 0.15625, ((0, 16), (2, 16))),
        "tendencies": scatter_about(streams_of[6], (MEMBERS, NLAT, NLON), 1.0, 6.0, ((0, 16), (1, 16))),
    }


clip_level = 0.9

def basis_table(wavenumber, lon_count):
    longitude = lax.broadcasted_iota(jnp.int32, (wavenumber.shape[0], lon_count), 1)
    phases = wavenumber[:, None] * longitude % lon_count
    angles = phases.astype(jnp.float32) * (2.0 * math.pi / lon_count)
    stacked = jnp.stack([jnp.cos(angles), -jnp.sin(angles)], axis=1)
    return stacked.reshape(2 * wavenumber.shape[0], lon_count).astype(jnp.bfloat16)

def reference(ar_state, forcing, ar_decay, amplitude, wavenumber, tables, tendencies):
    degree_grid = lax.broadcasted_iota(jnp.int32, (MWIN, NDEG), 1)
    kept_mask = (degree_grid >= wavenumber[:, None]).astype(jnp.float32)
    updated = ar_decay[:, None, None, None, None] * ar_state + amplitude[:, None, None, None, :] * forcing
    new_state = kept_mask[None, None, :, None, :] * updated
    coefficients = lax.optimization_barrier(jnp.sum(new_state, axis=0)).astype(jnp.bfloat16)

    def per_wave(index):
        block_rows = lax.dynamic_index_in_dim(coefficients, index, 1, keepdims=False)
        wave_table = lax.dynamic_index_in_dim(tables, index, 0, keepdims=False)
        product = jnp.dot(block_rows.reshape(2 * MEMBERS, NDEG), wave_table, preferred_element_type=jnp.float32)
        return product.reshape(MEMBERS, 2, NLAT)
    fourier = lax.map(per_wave, jnp.arange(MWIN, dtype=jnp.int32))
    fourier = jnp.transpose(fourier, (1, 3, 0, 2)).astype(jnp.bfloat16)
    basis = basis_table(wavenumber, NLON)

    def per_member(pair):
        member_rows, member_tend = pair
        pattern = jnp.dot(member_rows.reshape(NLAT, 2 * MWIN), basis, preferred_element_type=jnp.float32)
        pattern = jnp.clip(pattern * (1.0 / math.sqrt(MWIN)), -clip_level, clip_level)
        return (member_tend.astype(jnp.float32) * (1.0 + pattern)).astype(jnp.bfloat16)
    perturbed = lax.map(per_member, (fourier, tendencies))
    return (perturbed, new_state)
```

```python
import functools
import math

import jax
import jax.numpy as jnp
from jax import lax
from jax.experimental import pallas as pl
from jax.experimental.pallas import tpu as pltpu
from jax.sharding import PartitionSpec as P

clip_level = 0.9
cores = 2
contract_last = (((1,), (1,)), ((), ()))
contract_first = (((0,), (0,)), ((), ()))
megabyte = 1 << 20


def ring_shift(mesh_size, shift):
    chips = mesh_size // cores
    return [
        (z * cores + c, ((z + shift) % chips) * cores + c) for z in range(chips) for c in range(cores)
    ]


def core_swap(mesh_size):
    return [(m, m ^ 1) for m in range(mesh_size)]


def update_kernel(wave_ref, decay_ref, amplitude_ref, state_ref, forcing_ref, new_ref, coef_ref):
    step = pl.program_id(0)
    scales, members, waves, parts, degrees = state_ref.shape
    total_waves = waves * pl.num_programs(0)
    degree = lax.broadcasted_iota(jnp.int32, (parts, degrees), 1)
    for j in range(waves):
        first = wave_ref[lax.axis_index("ma") * total_waves + step * waves + j]
        kept = degree >= first
        rows = []
        for b in range(members):
            total = None
            for s in range(scales):
                value = (
                    decay_ref[s] * state_ref[s, b, j]
                    + amplitude_ref[s : s + 1, :] * forcing_ref[s, b, j]
                )
                value = jnp.where(kept, value, 0.0)
                new_ref[s, b, j] = value
                total = value if total is None else total + value
            rows.append(total)
        coef_ref[j] = jnp.concatenate(rows, axis=0).astype(jnp.bfloat16)


def update(wavenumber, ar_decay, amplitude, ar_state, forcing):
    scales, members, waves, parts, degrees = ar_state.shape
    per_step = 2
    block = pl.BlockSpec(
        (scales, members, per_step, parts, degrees), lambda i: (0, 0, i, 0, 0)
    )
    return pl.pallas_call(
        update_kernel,
        grid=(waves // per_step,),
        in_specs=[
            pl.BlockSpec(memory_space=pltpu.SMEM),
            pl.BlockSpec(memory_space=pltpu.SMEM),
            pl.BlockSpec((scales, degrees), lambda i: (0, 0)),
            block,
            block,
        ],
        out_specs=[
            block,
            pl.BlockSpec((per_step, members * parts, degrees), lambda i: (i, 0, 0)),
        ],
        out_shape=[
            jax.ShapeDtypeStruct(ar_state.shape, jnp.float32),
            jax.ShapeDtypeStruct((waves, members * parts, degrees), jnp.bfloat16),
        ],
        compiler_params=pltpu.CompilerParams(vmem_limit_bytes=16 * megabyte),
        name="update",
    )(wavenumber, ar_decay, amplitude, ar_state, forcing)


def legendre_kernel(layout, members, own_ref, other_ref, *refs):
    blocks = refs[: sum(layout)]
    outs = refs[sum(layout) : -1]
    stage = refs[-1]
    waves, lats, _ = own_ref.shape
    core = lax.axis_index("mem") % cores
    at = 0
    for count, out_ref in zip(layout, outs):
        pieces = blocks[at : at + count]
        at += count
        for j in range(waves):
            piece = pieces[j // (waves // count)]
            rows = piece[j % (waves // count)]
            for side, table_ref in enumerate((own_ref, other_ref)):
                product = lax.dot_general(
                    rows, table_ref[j], contract_last, preferred_element_type=jnp.float32
                )
                for b in range(members):
                    for c in range(2):
                        stage[side, c * waves + j, b * lats : (b + 1) * lats] = product[2 * b + c]
        out_ref[core] = stage[0].astype(jnp.bfloat16)
        out_ref[1 - core] = stage[1].astype(jnp.bfloat16)


def legendre(tables, blocks, members):
    waves, lats, degrees = tables[0].shape
    layout = tuple(len(b) for b in blocks)
    flat = [piece for b in blocks for piece in b]
    whole = pl.BlockSpec(memory_space=pltpu.VMEM)
    shape = (cores, 2 * waves, members * lats)
    return pl.pallas_call(
        functools.partial(legendre_kernel, layout, members),
        in_specs=[whole] * (2 + len(flat)),
        out_specs=[whole] * len(blocks),
        out_shape=[jax.ShapeDtypeStruct(shape, jnp.bfloat16)] * len(blocks),
        scratch_shapes=[pltpu.VMEM(shape, jnp.float32)],
        compiler_params=pltpu.CompilerParams(vmem_limit_bytes=16 * megabyte),
        cost_estimate=pl.CostEstimate(
            flops=len(blocks) * 1_000_000_000, bytes_accessed=4 * megabyte, transcendentals=0
        ),
        name="legendre",
    )(*tables, *flat)


def arrange_kernel(*refs):
    pieces, out_ref = refs[:-1], refs[-1]
    chips = len(pieces)
    here = lax.axis_index("mem") // cores
    for d, piece in enumerate(pieces):
        there = lax.rem(here + d, chips)
        for c in range(cores):
            out_ref[there * cores + c] = piece[c]


def arrange(pieces):
    whole = pl.BlockSpec(memory_space=pltpu.VMEM)
    _, rows, columns = pieces[0].shape
    return pl.pallas_call(
        arrange_kernel,
        in_specs=[whole] * len(pieces),
        out_specs=whole,
        out_shape=jax.ShapeDtypeStruct((len(pieces) * cores, rows, columns), jnp.bfloat16),
        compiler_params=pltpu.CompilerParams(vmem_limit_bytes=4 * megabyte),
        name="arrange",
    )(*pieces)


def basis_kernel(owners, wave_ref, out_ref):
    window, lanes = wave_ref.shape[0], 128
    lon_count = out_ref.shape[1]
    waves = window // owners
    tiles = lon_count // lanes
    wave = wave_ref[...]
    lane = lax.broadcasted_iota(jnp.int32, (window, lanes), 1)
    turn = 2.0 * math.pi / lon_count
    fine = (lax.rem(wave * lane, lon_count)).astype(jnp.float32) * turn
    coarse = (lax.rem(wave * lanes * lane, lon_count)).astype(jnp.float32) * turn
    cos_fine, sin_fine = jnp.cos(fine), jnp.sin(fine)
    cos_coarse, sin_coarse = jnp.cos(coarse), jnp.sin(coarse)
    for t in range(tiles):
        ca, sa = cos_coarse[:, t : t + 1], sin_coarse[:, t : t + 1]
        cosine = ca * cos_fine - sa * sin_fine
        minus_sine = -(sa * cos_fine + ca * sin_fine)
        for a in range(owners):
            rows = slice(a * waves, (a + 1) * waves)
            both = jnp.concatenate([cosine[rows], minus_sine[rows]], axis=0)
            out_ref[2 * a * waves : 2 * (a + 1) * waves, t * lanes : (t + 1) * lanes] = both.astype(
                jnp.bfloat16
            )


def basis_table(wavenumber, lon_count, owners):
    window = wavenumber.shape[0]
    return pl.pallas_call(
        functools.partial(basis_kernel, owners),
        in_specs=[pl.BlockSpec(memory_space=pltpu.VMEM)],
        out_specs=pl.BlockSpec(memory_space=pltpu.VMEM),
        out_shape=jax.ShapeDtypeStruct((2 * window, lon_count), jnp.bfloat16),
        compiler_params=pltpu.CompilerParams(vmem_limit_bytes=16 * megabyte),
        cost_estimate=pl.CostEstimate(
            flops=2_000_000_000, bytes_accessed=3 * megabyte, transcendentals=65536
        ),
        name="basis",
    )(wavenumber.reshape(window, 1))


def grid_kernel(scale, rows_ref, basis_ref, tend_ref, out_ref):
    pattern = lax.dot_general(
        rows_ref[...], basis_ref[...], contract_first, preferred_element_type=jnp.float32
    )
    pattern = jnp.clip(pattern * scale, -clip_level, clip_level)
    out_ref[...] = (tend_ref[...].astype(jnp.float32) * (1.0 + pattern)).astype(jnp.bfloat16)


def to_grid(rows, basis, tendencies, scale):
    members, lats, lons = tendencies.shape
    depth, height = rows.shape
    tile = 1024
    column = pl.BlockSpec((height, tile), lambda i: (0, i))
    out = pl.pallas_call(
        functools.partial(grid_kernel, scale),
        grid=(lons // tile,),
        in_specs=[
            pl.BlockSpec((depth, height), lambda i: (0, 0)),
            pl.BlockSpec((depth, tile), lambda i: (0, i)),
            column,
        ],
        out_specs=column,
        out_shape=jax.ShapeDtypeStruct((height, lons), jnp.bfloat16),
        compiler_params=pltpu.CompilerParams(vmem_limit_bytes=24 * megabyte),
        name="grid",
    )(rows, basis, tendencies.reshape(height, lons))
    return out.reshape(tendencies.shape)


def per_device(
    mem_size, ma_size, ar_state, forcing, ar_decay, amplitude, wavenumber, tables, tendencies
):
    members, waves = ar_state.shape[1], ar_state.shape[2]
    chips = mem_size // cores
    half = chips // 2
    own_table = jnp.swapaxes(tables, 1, 2)
    other_table = lax.ppermute(own_table, "mem", core_swap(mem_size))
    new_state, block = update(wavenumber, ar_decay, amplitude, ar_state, forcing)

    def shifted(value, shift):
        return lax.ppermute(value, "mem", ring_shift(mem_size, shift))

    both = (own_table, other_table)
    basis = basis_table(wavenumber, tendencies.shape[2], ma_size)
    returned = [None] * chips
    ahead = behind = block
    pending = [((block,), 0)]
    for step in range(1, half + 1):
        if step < half:
            ahead, behind = shifted(ahead, 1), shifted(behind, -1)
            arrived = [((ahead,), step), ((behind,), chips - step)]
        else:
            ahead, behind = shifted(ahead[: waves // 2], 1), shifted(behind[waves // 2 :], -1)
            arrived = [((ahead, behind), half)]
        results = legendre(both, [p for p, _ in pending], members)
        for (_, d), result in zip(pending, results):
            returned[d] = shifted(result, -d) if d else result
        pending = arrived
    results = legendre(both, [p for p, _ in pending], members)
    for (_, d), result in zip(pending, results):
        returned[d] = shifted(result, -d)
    ordered = arrange(returned)
    spread = lax.all_to_all(ordered, "ma", split_axis=0, concat_axis=0, tiled=True)
    rows = spread.reshape(-1, spread.shape[2])
    window = wavenumber.shape[0]
    perturbed = to_grid(rows, basis, tendencies, 1.0 / math.sqrt(window))
    return (perturbed, new_state)


def solution(mesh):
    return jax.shard_map(
        functools.partial(per_device, mesh.shape["mem"], mesh.shape["ma"]),
        mesh=mesh,
        in_specs=(
            P(None, "mem", "ma", None, None),
            P(None, "mem", "ma", None, None),
            P(),
            P(),
            P(),
            P("ma", None, "mem"),
            P("mem", "ma", None),
        ),
        out_specs=(P("mem", "ma", None), P(None, "mem", "ma", None, None)),
        check_vma=False,
    )
```

```python
import functools
import math

import jax
import jax.numpy as jnp
from jax import lax
from jax.experimental import pallas as pl
from jax.experimental.pallas import tpu as pltpu
from jax.sharding import PartitionSpec as P

clip_level = 0.9
cores = 2
contract_last = (((1,), (1,)), ((), ()))
contract_first = (((0,), (0,)), ((), ()))
megabyte = 1 << 20


def ring_shift(mesh_size, shift):
    chips = mesh_size // cores
    return [
        (z * cores + c, ((z + shift) % chips) * cores + c) for z in range(chips) for c in range(cores)
    ]


def in_hbm(value):
    return pltpu.with_memory_space_constraint(value, pltpu.HBM)


def core_swap(mesh_size):
    return [(m, m ^ 1) for m in range(mesh_size)]


def update_kernel(
    wave_ref, decay_ref, amplitude_ref, state_hbm, forcing_hbm, new_hbm, *refs
):
    coef_refs, (state_ref, forcing_ref, new_ref, in_sems, out_sems) = refs[:2], refs[2:]
    scales, members, waves, parts, degrees = state_ref.shape
    chunks = in_sems.shape[1]
    size = waves // chunks
    loads, stores = [], []
    for i in range(chunks):
        at = (slice(None), slice(None), pl.ds(i * size, size))
        loads.append(
            [
                pltpu.make_async_copy(hbm.at[at], ref.at[at], in_sems.at[k, i])
                for k, (hbm, ref) in enumerate(((state_hbm, state_ref), (forcing_hbm, forcing_ref)))
            ]
        )
        stores.append(pltpu.make_async_copy(new_ref.at[at], new_hbm.at[at], out_sems.at[i]))
        for copy in loads[-1]:
            copy.start()
    degree = lax.broadcasted_iota(jnp.int32, (parts, degrees), 1)
    here = lax.axis_index("ma") * waves
    for i in range(chunks):
        for copy in loads[i]:
            copy.wait()
        for j in range(i * size, (i + 1) * size):
            kept = degree >= wave_ref[here + j]
            rows = []
            for b in range(members):
                total = None
                for s in range(scales):
                    value = (
                        decay_ref[s] * state_ref[s, b, j]
                        + amplitude_ref[s : s + 1, :] * forcing_ref[s, b, j]
                    )
                    value = jnp.where(kept, value, 0.0)
                    new_ref[s, b, j] = value
                    total = value if total is None else total + value
                rows.append(total)
            half = waves // len(coef_refs)
            coef_refs[j // half][j % half] = jnp.concatenate(rows, axis=0).astype(jnp.bfloat16)
        stores[i].start()
    for copy in stores:
        copy.wait()


def update(wavenumber, ar_decay, amplitude, ar_state, forcing):
    scales, members, waves, parts, degrees = ar_state.shape
    chunks, halves = 4, 2
    far = pl.BlockSpec(memory_space=pltpu.HBM)
    near = pl.BlockSpec(memory_space=pltpu.VMEM)
    coef = jax.ShapeDtypeStruct((waves // halves, members * parts, degrees), jnp.bfloat16)
    return pl.pallas_call(
        update_kernel,
        in_specs=[
            pl.BlockSpec(memory_space=pltpu.SMEM),
            pl.BlockSpec(memory_space=pltpu.SMEM),
            near,
            far,
            far,
        ],
        out_specs=[far] + [near] * halves,
        out_shape=[jax.ShapeDtypeStruct(ar_state.shape, jnp.float32)] + [coef] * halves,
        scratch_shapes=[pltpu.VMEM(ar_state.shape, jnp.float32)] * 3
        + [pltpu.SemaphoreType.DMA((2, chunks)), pltpu.SemaphoreType.DMA((chunks,))],
        compiler_params=pltpu.CompilerParams(vmem_limit_bytes=12 * megabyte),
        name="update",
    )(*(in_hbm(x) for x in (wavenumber, ar_decay, amplitude, ar_state, forcing)))


def legendre_kernel(layout, members, own_ref, other_ref, *refs):
    halves = len(layout)
    blocks, out_ref, stage = refs[:-2], refs[-2], refs[-1]
    waves, lats, _ = own_ref.shape
    chips = out_ref.shape[0]
    half = waves // halves
    core = lax.axis_index("mem") % cores
    here = lax.axis_index("mem") // cores
    rows = 2 * members
    for h, offsets in enumerate(layout):
        pieces = blocks[h * chips : (h + 1) * chips]
        for i in range(half):
            j = h * half + i
            lhs = jnp.concatenate([piece[i] for piece in pieces], axis=0)
            for side, table_ref in enumerate((own_ref, other_ref)):
                product = lax.dot_general(
                    lhs, table_ref[j], contract_last, preferred_element_type=jnp.float32
                )
                for n in range(chips):
                    for b in range(members):
                        for c in range(2):
                            r = n * rows + 2 * b + c
                            stage[n, side, c * waves + j, b * lats : (b + 1) * lats] = product[r]
    for n, offset in enumerate(layout[0]):
        there = lax.rem(here + chips - offset, chips)
        out_ref[there, core] = stage[n, 0].astype(jnp.bfloat16)
        out_ref[there, 1 - core] = stage[n, 1].astype(jnp.bfloat16)


def legendre(tables, layout, blocks, members):
    waves, lats, degrees = tables[0].shape
    chips = len(layout[0])
    whole = pl.BlockSpec(memory_space=pltpu.VMEM)
    shape = (chips, cores, 2 * waves, members * lats)
    return pl.pallas_call(
        functools.partial(legendre_kernel, layout, members),
        in_specs=[whole] * (2 + len(blocks)),
        out_specs=whole,
        out_shape=jax.ShapeDtypeStruct(shape, jnp.bfloat16),
        scratch_shapes=[pltpu.VMEM(shape, jnp.float32)],
        compiler_params=pltpu.CompilerParams(vmem_limit_bytes=8 * megabyte),
        cost_estimate=pl.CostEstimate(
            flops=4_000_000_000, bytes_accessed=4 * megabyte, transcendentals=0
        ),
        name="legendre",
    )(*tables, *blocks)


def basis_kernel(owners, wave_ref, out_ref):
    window, lanes = wave_ref.shape[0], 128
    lon_count = out_ref.shape[1]
    waves = window // owners
    tiles = lon_count // lanes
    wave = wave_ref[...]
    lane = lax.broadcasted_iota(jnp.int32, (window, lanes), 1)
    turn = 2.0 * math.pi / lon_count
    fine = (lax.rem(wave * lane, lon_count)).astype(jnp.float32) * turn
    coarse = (lax.rem(wave * lanes * lane, lon_count)).astype(jnp.float32) * turn
    cos_fine, sin_fine = jnp.cos(fine), jnp.sin(fine)
    cos_coarse, sin_coarse = jnp.cos(coarse), jnp.sin(coarse)
    for t in range(tiles):
        ca, sa = cos_coarse[:, t : t + 1], sin_coarse[:, t : t + 1]
        cosine = ca * cos_fine - sa * sin_fine
        minus_sine = -(sa * cos_fine + ca * sin_fine)
        for a in range(owners):
            rows = slice(a * waves, (a + 1) * waves)
            both = jnp.concatenate([cosine[rows], minus_sine[rows]], axis=0)
            out_ref[2 * a * waves : 2 * (a + 1) * waves, t * lanes : (t + 1) * lanes] = both.astype(
                jnp.bfloat16
            )


def basis_table(wavenumber, lon_count, owners):
    window = wavenumber.shape[0]
    return pl.pallas_call(
        functools.partial(basis_kernel, owners),
        in_specs=[pl.BlockSpec(memory_space=pltpu.VMEM)],
        out_specs=pl.BlockSpec(memory_space=pltpu.VMEM),
        out_shape=jax.ShapeDtypeStruct((2 * window, lon_count), jnp.bfloat16),
        compiler_params=pltpu.CompilerParams(vmem_limit_bytes=6 * megabyte),
        cost_estimate=pl.CostEstimate(
            flops=2_000_000_000, bytes_accessed=3 * megabyte, transcendentals=65536
        ),
        name="basis",
    )(wavenumber.reshape(window, 1))


def grid_kernel(scale, rows_ref, basis_ref, tend_ref, out_ref):
    pattern = lax.dot_general(
        rows_ref[...], basis_ref[...], contract_first, preferred_element_type=jnp.float32
    )
    pattern = jnp.clip(pattern * scale, -clip_level, clip_level)
    out_ref[...] = (tend_ref[...].astype(jnp.float32) * (1.0 + pattern)).astype(jnp.bfloat16)


def to_grid(rows, basis, tendencies, scale):
    members, lats, lons = tendencies.shape
    depth, height = rows.shape
    tile = 1024
    column = pl.BlockSpec((height, tile), lambda i: (0, i))
    out = pl.pallas_call(
        functools.partial(grid_kernel, scale),
        grid=(lons // tile,),
        in_specs=[
            pl.BlockSpec((depth, height), lambda i: (0, 0)),
            pl.BlockSpec((depth, tile), lambda i: (0, i)),
            column,
        ],
        out_specs=column,
        out_shape=jax.ShapeDtypeStruct((height, lons), jnp.bfloat16),
        compiler_params=pltpu.CompilerParams(vmem_limit_bytes=10 * megabyte),
        name="grid",
    )(rows, basis, tendencies.reshape(height, lons))
    return out.reshape(tendencies.shape)


def per_device(
    mem_size, ma_size, ar_state, forcing, ar_decay, amplitude, wavenumber, tables, tendencies
):
    members, waves = ar_state.shape[1], ar_state.shape[2]
    chips = mem_size // cores
    own_table = jnp.swapaxes(tables, 1, 2)
    other_table = lax.ppermute(own_table, "mem", core_swap(mem_size))
    other_table = pltpu.with_memory_space_constraint(other_table, pltpu.VMEM)
    new_state, *halves = update(wavenumber, ar_decay, amplitude, ar_state, forcing)
    basis = basis_table(wavenumber, tendencies.shape[2], ma_size)

    held = [{0: block} for block in halves]
    ahead, behind = list(halves), list(halves)
    for step in range(1, chips // 2 + 1):
        for h in range(2):
            if step < chips // 2 or h == 0:
                ahead[h] = lax.ppermute(ahead[h], "mem", ring_shift(mem_size, 1))
                held[h][step] = ahead[h]
            if step < chips // 2 or h == 1:
                behind[h] = lax.ppermute(behind[h], "mem", ring_shift(mem_size, -1))
                held[h][chips - step] = behind[h]
        if step == 1:
            ahead, behind, basis = lax.optimization_barrier((ahead, behind, basis))
    offsets = tuple(range(chips))
    blocks = [held[h][d] for h in range(2) for d in offsets]
    product = legendre((own_table, other_table), (offsets, offsets), blocks, members)
    groups = [[z * cores + c for z in range(chips)] for c in range(cores)]
    product = lax.all_to_all(
        product, "mem", split_axis=0, concat_axis=0, axis_index_groups=groups, tiled=True
    )
    product = product.reshape(mem_size, *product.shape[2:])
    spread = lax.all_to_all(product, "ma", split_axis=0, concat_axis=0, tiled=True)
    rows = spread.reshape(-1, spread.shape[2])
    window = wavenumber.shape[0]
    perturbed = to_grid(rows, basis, tendencies, 1.0 / math.sqrt(window))
    return (perturbed, new_state)


def solution(mesh):
    return jax.shard_map(
        functools.partial(per_device, mesh.shape["mem"], mesh.shape["ma"]),
        mesh=mesh,
        in_specs=(
            P(None, "mem", "ma", None, None),
            P(None, "mem", "ma", None, None),
            P(),
            P(),
            P(),
            P("ma", None, "mem"),
            P("mem", "ma", None),
        ),
        out_specs=(P("mem", "ma", None), P(None, "mem", "ma", None, None)),
        check_vma=False,
    )
```

```python
import functools
import math

import jax
import jax.numpy as jnp
from jax import lax
from jax.experimental import pallas as pl
from jax.experimental.pallas import tpu as pltpu
from jax.sharding import PartitionSpec as P

clip_level = 0.9
cores = 2
contract_last = (((1,), (1,)), ((), ()))
contract_first = (((0,), (0,)), ((), ()))
megabyte = 1 << 20


def ring_shift(mesh_size, shift):
    chips = mesh_size // cores
    return [
        (z * cores + c, ((z + shift) % chips) * cores + c) for z in range(chips) for c in range(cores)
    ]


def in_hbm(value):
    return pltpu.with_memory_space_constraint(value, pltpu.HBM)


def core_swap(mesh_size):
    return [(m, m ^ 1) for m in range(mesh_size)]


def update_kernel(
    wave_hbm, decay_hbm, amplitude_hbm, state_hbm, forcing_hbm, new_hbm, *refs
):
    coef_refs, refs = refs[:2], refs[2:]
    wave_ref, decay_ref, amplitude_ref, state_ref, forcing_ref, new_ref = refs[:6]
    small_sems, in_sems, out_sems = refs[6:]
    scales, members, waves, parts, degrees = state_ref.shape
    chunks = in_sems.shape[1]
    size = waves // chunks
    small = [
        pltpu.make_async_copy(hbm, ref, small_sems.at[k])
        for k, (hbm, ref) in enumerate(
            ((wave_hbm, wave_ref), (decay_hbm, decay_ref), (amplitude_hbm, amplitude_ref))
        )
    ]
    for copy in small:
        copy.start()
    loads, stores = [], []
    for i in range(chunks):
        at = (slice(None), slice(None), pl.ds(i * size, size))
        loads.append(
            [
                pltpu.make_async_copy(hbm.at[at], ref.at[at], in_sems.at[k, i])
                for k, (hbm, ref) in enumerate(((state_hbm, state_ref), (forcing_hbm, forcing_ref)))
            ]
        )
        stores.append(pltpu.make_async_copy(new_ref.at[at], new_hbm.at[at], out_sems.at[i]))
        for copy in loads[-1]:
            copy.start()
    degree = lax.broadcasted_iota(jnp.int32, (parts, degrees), 1)
    here = lax.axis_index("ma") * waves
    for copy in small:
        copy.wait()
    decay = [decay_ref[s] for s in range(scales)]
    amplitude = [
        jnp.broadcast_to(amplitude_ref[s : s + 1, :], (parts, degrees)) for s in range(scales)
    ]
    for i in range(chunks):
        for copy in loads[i]:
            copy.wait()
        for j in range(i * size, (i + 1) * size):
            kept = degree >= wave_ref[here + j]
            rows = []
            for b in range(members):
                total = None
                for s in range(scales):
                    value = decay[s] * state_ref[s, b, j] + amplitude[s] * forcing_ref[s, b, j]
                    value = jnp.where(kept, value, 0.0)
                    new_ref[s, b, j] = value
                    total = value if total is None else total + value
                rows.append(total)
            half = waves // len(coef_refs)
            coef_refs[j // half][j % half] = jnp.concatenate(rows, axis=0).astype(jnp.bfloat16)
        stores[i].start()
    for copy in stores:
        copy.wait()


def update(wavenumber, ar_decay, amplitude, ar_state, forcing):
    scales, members, waves, parts, degrees = ar_state.shape
    chunks, halves = 4, 2
    far = pl.BlockSpec(memory_space=pltpu.HBM)
    near = pl.BlockSpec(memory_space=pltpu.VMEM)
    coef = jax.ShapeDtypeStruct((waves // halves, members * parts, degrees), jnp.bfloat16)
    return pl.pallas_call(
        update_kernel,
        in_specs=[far] * 5,
        out_specs=[far] + [near] * halves,
        out_shape=[jax.ShapeDtypeStruct(ar_state.shape, jnp.float32)] + [coef] * halves,
        scratch_shapes=[
            pltpu.SMEM(wavenumber.shape, jnp.int32),
            pltpu.SMEM(ar_decay.shape, jnp.float32),
            pltpu.VMEM(amplitude.shape, jnp.float32),
        ]
        + [pltpu.VMEM(ar_state.shape, jnp.float32)] * 3
        + [
            pltpu.SemaphoreType.DMA((3,)),
            pltpu.SemaphoreType.DMA((2, chunks)),
            pltpu.SemaphoreType.DMA((chunks,)),
        ],
        compiler_params=pltpu.CompilerParams(vmem_limit_bytes=12 * megabyte),
        name="update",
    )(*(in_hbm(x) for x in (wavenumber, ar_decay, amplitude, ar_state, forcing)))


def legendre_kernel(layout, members, own_ref, other_ref, *refs):
    halves = len(layout)
    blocks, out_ref, stage = refs[:-2], refs[-2], refs[-1]
    waves, lats, _ = own_ref.shape
    chips = out_ref.shape[0]
    half = waves // halves
    core = lax.axis_index("mem") % cores
    here = lax.axis_index("mem") // cores
    rows = 2 * members
    for h, offsets in enumerate(layout):
        pieces = blocks[h * chips : (h + 1) * chips]
        for i in range(half):
            j = h * half + i
            lhs = jnp.concatenate([piece[i] for piece in pieces], axis=0)
            for side, table_ref in enumerate((own_ref, other_ref)):
                product = lax.dot_general(
                    lhs, table_ref[j], contract_last, preferred_element_type=jnp.float32
                )
                for n in range(chips):
                    for b in range(members):
                        for c in range(2):
                            r = n * rows + 2 * b + c
                            stage[n, side, c * waves + j, b * lats : (b + 1) * lats] = product[r]
    for n, offset in enumerate(layout[0]):
        there = lax.rem(here + chips - offset, chips)
        out_ref[there, core] = stage[n, 0].astype(jnp.bfloat16)
        out_ref[there, 1 - core] = stage[n, 1].astype(jnp.bfloat16)


def legendre(tables, layout, blocks, members):
    waves, lats, degrees = tables[0].shape
    chips = len(layout[0])
    whole = pl.BlockSpec(memory_space=pltpu.VMEM)
    shape = (chips, cores, 2 * waves, members * lats)
    return pl.pallas_call(
        functools.partial(legendre_kernel, layout, members),
        in_specs=[whole] * (2 + len(blocks)),
        out_specs=whole,
        out_shape=jax.ShapeDtypeStruct(shape, jnp.bfloat16),
        scratch_shapes=[pltpu.VMEM(shape, jnp.float32)],
        compiler_params=pltpu.CompilerParams(vmem_limit_bytes=8 * megabyte),
        cost_estimate=pl.CostEstimate(
            flops=4_000_000_000, bytes_accessed=4 * megabyte, transcendentals=0
        ),
        name="legendre",
    )(*tables, *blocks)


def basis_kernel(owners, wave_ref, out_ref):
    window, lanes = wave_ref.shape[1], 128
    lon_count = out_ref.shape[1]
    waves = window // owners
    tiles = lon_count // lanes
    wave = jnp.transpose(jnp.broadcast_to(wave_ref[...], (lanes, window)))
    lane = lax.broadcasted_iota(jnp.int32, (window, lanes), 1)
    turn = 2.0 * math.pi / lon_count
    fine = (lax.rem(wave * lane, lon_count)).astype(jnp.float32) * turn
    coarse = (lax.rem(wave * lanes * lane, lon_count)).astype(jnp.float32) * turn
    cos_fine, sin_fine = jnp.cos(fine), jnp.sin(fine)
    cos_coarse, sin_coarse = jnp.cos(coarse), jnp.sin(coarse)
    for t in range(tiles):
        ca, sa = cos_coarse[:, t : t + 1], sin_coarse[:, t : t + 1]
        cosine = ca * cos_fine - sa * sin_fine
        minus_sine = -(sa * cos_fine + ca * sin_fine)
        for a in range(owners):
            rows = slice(a * waves, (a + 1) * waves)
            both = jnp.concatenate([cosine[rows], minus_sine[rows]], axis=0)
            out_ref[2 * a * waves : 2 * (a + 1) * waves, t * lanes : (t + 1) * lanes] = both.astype(
                jnp.bfloat16
            )


def basis_table(wavenumber, lon_count, owners):
    window = wavenumber.shape[0]
    return pl.pallas_call(
        functools.partial(basis_kernel, owners),
        in_specs=[pl.BlockSpec(memory_space=pltpu.VMEM)],
        out_specs=pl.BlockSpec(memory_space=pltpu.VMEM),
        out_shape=jax.ShapeDtypeStruct((2 * window, lon_count), jnp.bfloat16),
        compiler_params=pltpu.CompilerParams(vmem_limit_bytes=6 * megabyte),
        cost_estimate=pl.CostEstimate(
            flops=2_000_000_000, bytes_accessed=3 * megabyte, transcendentals=65536
        ),
        name="basis",
    )(wavenumber.reshape(1, window))


def grid_kernel(scale, rows_ref, basis_ref, tend_ref, out_hbm, stage, sems):
    height, lons = stage.shape
    tiles = sems.shape[0]
    tile = lons // tiles
    rows = jnp.transpose(rows_ref[...].astype(jnp.float32)).astype(jnp.bfloat16)
    copies = []
    for i in range(tiles):
        at = (slice(None), pl.ds(i * tile, tile))
        pattern = jnp.dot(rows, basis_ref[at], preferred_element_type=jnp.float32)
        pattern = jnp.clip(pattern * scale, -clip_level, clip_level)
        stage[at] = (tend_ref[at].astype(jnp.float32) * (1.0 + pattern)).astype(jnp.bfloat16)
        copies.append(pltpu.make_async_copy(stage.at[at], out_hbm.at[at], sems.at[i]))
        copies[-1].start()
    for copy in copies:
        copy.wait()


def to_grid(rows, basis, tendencies, scale):
    members, lats, lons = tendencies.shape
    height = rows.shape[1]
    tiles = 10
    near = pl.BlockSpec(memory_space=pltpu.VMEM)
    out = pl.pallas_call(
        functools.partial(grid_kernel, scale),
        in_specs=[near] * 3,
        out_specs=pl.BlockSpec(memory_space=pltpu.HBM),
        out_shape=jax.ShapeDtypeStruct((height, lons), jnp.bfloat16),
        scratch_shapes=[
            pltpu.VMEM((height, lons), jnp.bfloat16),
            pltpu.SemaphoreType.DMA((tiles,)),
        ],
        compiler_params=pltpu.CompilerParams(vmem_limit_bytes=12 * megabyte),
        name="grid",
    )(rows, basis, tendencies.reshape(height, lons))
    return out.reshape(tendencies.shape)


def per_device(
    mem_size, ma_size, ar_state, forcing, ar_decay, amplitude, wavenumber, tables, tendencies
):
    members, waves = ar_state.shape[1], ar_state.shape[2]
    chips = mem_size // cores
    own_table = jnp.swapaxes(tables, 1, 2)
    other_table = lax.ppermute(own_table, "mem", core_swap(mem_size))
    other_table = pltpu.with_memory_space_constraint(other_table, pltpu.VMEM)
    new_state, *halves = update(wavenumber, ar_decay, amplitude, ar_state, forcing)

    def shifted(value, shift):
        return lax.ppermute(value, "mem", ring_shift(mem_size, shift))

    held = [{0: block} for block in halves]
    furthest = chips // 2
    for step in range(1, furthest):
        for h, way in ((0, 1), (1, -1), (1, 1), (0, -1)):
            last = held[h][way * (step - 1) % chips]
            if step == furthest - 1 and h == (way < 0):
                held[h][furthest] = shifted(last, 2 * way)
            held[h][way * step % chips] = shifted(last, way)
    late, timed = lax.optimization_barrier((held[0][chips - 2], wavenumber))
    held[0][chips - 2] = late
    basis = basis_table(timed, tendencies.shape[2], ma_size)
    held[1][furthest], basis = lax.optimization_barrier((held[1][furthest], basis))
    offsets = tuple(range(chips))
    blocks = [held[h][d] for h in range(2) for d in offsets]
    product = legendre((own_table, other_table), (offsets, offsets), blocks, members)
    groups = [[z * cores + c for z in range(chips)] for c in range(cores)]
    product = lax.all_to_all(
        product, "mem", split_axis=0, concat_axis=0, axis_index_groups=groups, tiled=True
    )
    product = product.reshape(mem_size, *product.shape[2:])
    spread = lax.all_to_all(product, "ma", split_axis=0, concat_axis=0, tiled=True)
    rows = spread.reshape(-1, spread.shape[2])
    window = wavenumber.shape[0]
    perturbed = to_grid(rows, basis, tendencies, 1.0 / math.sqrt(window))
    return (perturbed, new_state)


def solution(mesh):
    return jax.shard_map(
        functools.partial(per_device, mesh.shape["mem"], mesh.shape["ma"]),
        mesh=mesh,
        in_specs=(
            P(None, "mem", "ma", None, None),
            P(None, "mem", "ma", None, None),
            P(),
            P(),
            P(),
            P("ma", None, "mem"),
            P("mem", "ma", None),
        ),
        out_specs=(P("mem", "ma", None), P(None, "mem", "ma", None, None)),
        check_vma=False,
    )
```
